512 devices in a mesh: batch: 64 (over z, y), tensor: 4 (over x), section: 2 (over core).
Axes of the slice: x: 4, y: 8, z: 8, core: 2. Of those that a mesh axis runs over, the one named last changes fastest.
Arguments:
- prefill_cache: bfloat16 [2, 512, 2, 4, 256, 128], P('section', ('batch', 'tensor')), may hold values from -5 to 5
- lengths: int32 [256], P('batch'), may hold values from 1 to 1280, as said below
- page_table: int32 [256, 5], P('batch'), may hold values from -1 to 7, as said below
- holder: int32 [64, 8], replicated, may hold values from 0 to 63, as said below
- queries: bfloat16 [256, 2, 4, 32, 128], P(('batch', 'section'), None, None, 'tensor'), may hold values from -120 to 120
- new_kv: bfloat16 [256, 2, 4, 2, 4, 128], P(('batch', 'section'), None, None, None, 'tensor'), may hold values from -5 to 5
Outputs:
- attended: bfloat16 [256, 2, 4, 32, 128], P(('batch', 'section'), None, None, 'tensor')
- decode_pool: bfloat16 [2, 512, 2, 4, 256, 128], P('section', 'batch', None, 'tensor')
The draws below stay inside these ranges and needn't reach their ends.
Inputs may be any that keep to these rules, and one draw needn't show every extreme that they name: Request r's prompt has lengths[r] tokens, held in ceil(lengths[r] / 256) pages. `page_table`: row r names in its first ceil(lengths[r] / 256) columns the pool positions (0 to 7) of the request's pages in order, and -1 after; a position is named at most once among the 4 requests of one batch index; some batch index uses all 8 positions. holder[b, q] = b XOR key_q (bitwise exclusive or of the binary digits), where key_0 to key_7 are distinct numbers of 0 to 63; so each column is a permutation of the batch indices and each row names distinct ones.
All inputs are finite; a program needn't handle non-finite values.
Results may differ from the reference program's by a relative error of at most 0.0038.
Values may be sent and summed in bfloat16 or wider, within the bound.
No kernel may reach another device: no remote copies, remote signals or barrier semaphores. Data moves between devices by JAX's collectives and lax.ppermute only.
A program may use at most 64 MiB of HBM per device.

```python
import math
import jax
import jax.numpy as jnp
from jax import lax

HEAD = 128
KV_HEADS = 4
GROUP = 8
PAGE = 256
STEPS = 4
REQ_GRP = 4
LAYERS = 2
Q_HEADS = 32
POSITIONS = 8
REQUESTS = 256
MAX_PAGES = 5
N_BATCH = 64


def page_layout(key):
    base = jax.random.fold_in(key, 11)
    subkeys = jax.random.split(base, 6)
    spare = POSITIONS - REQ_GRP
    width = max(spare, 1)
    extra_total = jax.random.randint(subkeys[0], (N_BATCH,), 0, spare + 1)
    full_group = jax.random.randint(subkeys[5], (), 0, N_BATCH)
    full_request = jax.random.randint(jax.random.fold_in(base, 7), (), 0, REQ_GRP)
    group_ids = jnp.arange(N_BATCH, dtype=jnp.int32)
    request_ids = jnp.arange(REQ_GRP, dtype=jnp.int32)
    is_full = group_ids == full_group
    extra_total = jnp.where(is_full, spare, extra_total)
    target = jax.random.randint(subkeys[1], (N_BATCH, width), 0, REQ_GRP)
    target = jnp.where(is_full[:, None], full_request, target)
    active = jnp.arange(width, dtype=jnp.int32)[None, :] < extra_total[:, None]
    chosen = (target[:, :, None] == request_ids[None, None, :]) & active[:, :, None]
    counts = 1 + jnp.sum(chosen.astype(jnp.int32), axis=1)
    last_part = jax.random.randint(subkeys[2], (N_BATCH, REQ_GRP), 1, PAGE + 1)
    longest = is_full[:, None] & (request_ids[None, :] == full_request)
    last_part = jnp.where(longest, PAGE, last_part)
    lengths = (counts - 1) * PAGE + last_part
    ranking = jax.random.randint(subkeys[3], (N_BATCH, POSITIONS), 0, 1 << 20) * POSITIONS + jnp.arange(POSITIONS, dtype=jnp.int32)[None, :]
    order = jnp.argsort(ranking, axis=1).astype(jnp.int32)
    starts = jnp.cumsum(counts, axis=1) - counts
    column = jnp.arange(MAX_PAGES, dtype=jnp.int32)[None, None, :]
    index = jnp.clip(starts[:, :, None] + column, 0, POSITIONS - 1)
    picked = jnp.take_along_axis(jnp.broadcast_to(order[:, None, :], (N_BATCH, REQ_GRP, POSITIONS)), index, axis=2)
    table = jnp.where(column < counts[:, :, None], picked, -1)
    route_keys = jax.random.permutation(subkeys[4], N_BATCH)[:POSITIONS].astype(jnp.int32)
    holder = jnp.bitwise_xor(group_ids[:, None], route_keys[None, :])
    return (lengths.reshape(REQUESTS).astype(jnp.int32), table.reshape(REQUESTS, MAX_PAGES).astype(jnp.int32), holder.astype(jnp.int32))


def decode_inputs(key):
    base = jax.random.fold_in(key, 23)
    key_pairs, key_queries = jax.random.split(base, 2)
    new_kv = jnp.clip(jax.random.normal(key_pairs, (REQUESTS, LAYERS, STEPS, 2, KV_HEADS, HEAD), jnp.float32), -5.0, 5.0)
    shape = (REQUESTS, LAYERS, STEPS, KV_HEADS, GROUP, HEAD)
    queries = jnp.clip(jax.random.normal(key_queries, shape, jnp.float32), -5.0, 5.0)
    return (queries.reshape(REQUESTS, LAYERS, STEPS, KV_HEADS * GROUP, HEAD).astype(jnp.bfloat16), new_kv.astype(jnp.bfloat16))


def draw_lengths(key, part):
    return page_layout(key)[0]


def draw_page_table(key, part):
    return page_layout(key)[1]


def draw_holder(key, part):
    return page_layout(key)[2]


def draw_queries(key, part):
    return decode_inputs(key)[0]


def draw_new_kv(key, part):
    return decode_inputs(key)[1]


def block_scale(own_key, extent, shards, smallest, high):
    def one(dim, shards_of):
        draws = jax.random.uniform(jax.random.fold_in(jax.random.fold_in(own_key, 6), dim), (shards_of,), jnp.float32, smallest / len(shards), high / len(shards))
        return jnp.repeat(jnp.exp(draws), extent[dim] // shards_of).reshape((-1,) + (1,) * (len(extent) - dim - 1))

    level = one(*shards[0])
    for cut in shards[1:]:
        level = level * one(*cut)
    return level


def noise(key, extent, deviation, most, cuts=(), kind=jnp.bfloat16):
    factor_of = block_scale(key, extent, cuts, -0.22, 0.18) if cuts else 1.0
    drawn = jax.random.normal(key, extent, jnp.float32) * deviation * factor_of
    return jnp.minimum(jnp.maximum(drawn, -most), most).astype(kind)


def setup_inputs(seed: int = 0) -> dict:
    key_of = jax.random.split(jax.random.key(seed), 7)
    prefill_cache = noise(key_of[0], (LAYERS, N_BATCH * POSITIONS, 2, KV_HEADS, PAGE, HEAD), 1.0, 5.0, ((0, 2), (1, 256)))
    lengths = draw_lengths(jax.random.fold_in(key_of[6], 71), 0)
    page_table = draw_page_table(jax.random.fold_in(key_of[6], 71), 0)
    holder = draw_holder(jax.random.fold_in(key_of[6], 71), 0)
    queries = draw_queries(jax.random.fold_in(key_of[6], 71), 0)
    new_kv = draw_new_kv(jax.random.fold_in(key_of[6], 71), 0)
    return dict(prefill_cache=prefill_cache, lengths=lengths, page_table=page_table, holder=holder, queries=queries, new_kv=new_kv)


MASKED = -1e+30

def position_table(lengths, page_table):
    table_rows = page_table.reshape(N_BATCH, REQ_GRP, MAX_PAGES)
    slot_ids = jnp.arange(POSITIONS, dtype=jnp.int32)
    page_hits = (table_rows[:, :, :, None] == slot_ids).astype(jnp.int32)
    in_use = lax.optimization_barrier(jnp.sum(page_hits, axis=(1, 2))) > 0
    request_of = lax.optimization_barrier(jnp.sum(page_hits * jnp.arange(REQ_GRP, dtype=jnp.int32)[None, :, None, None], axis=(1, 2)))
    page_of = lax.optimization_barrier(jnp.sum(page_hits * jnp.arange(MAX_PAGES, dtype=jnp.int32)[None, None, :, None], axis=(1, 2)))
    length_of = lax.optimization_barrier(jnp.sum(page_hits * lengths.reshape(N_BATCH, REQ_GRP)[:, :, None, None], axis=(1, 2)))
    live_count = jnp.clip(length_of - page_of * PAGE, 0, PAGE)
    return (in_use, request_of, live_count)

def block_partials(queries_at, key_rows, value_rows, token_mask):
    score_scale = 1.0 / math.sqrt(HEAD)
    scores = jnp.einsum('nigex,ngpx->ngiep', queries_at.astype(jnp.float32), key_rows.astype(jnp.float32)) * score_scale
    page_peak = lax.optimization_barrier(jnp.max(jnp.where(token_mask, scores, MASKED), axis=-1))
    weights = jnp.where(token_mask, jnp.exp(scores - page_peak[..., None]), 0.0).astype(jnp.bfloat16)
    weight_sum = lax.optimization_barrier(jnp.sum(weights.astype(jnp.float32), axis=-1))
    page_output = jnp.einsum('ngiep,ngpx->ngiex', weights.astype(jnp.float32), value_rows.astype(jnp.float32))
    return (page_peak, weight_sum, page_output)

def reference(prefill_cache, lengths, page_table, holder, queries, new_kv):
    in_use, request_of, live_count = position_table(lengths, page_table)
    slot_ids = jnp.arange(POSITIONS, dtype=jnp.int32)
    batch_ids = jnp.broadcast_to(jnp.arange(N_BATCH, dtype=jnp.int32)[:, None], (N_BATCH, POSITIONS))
    sender_of = jnp.zeros((N_BATCH, POSITIONS), jnp.int32).at[holder, slot_ids[None, :]].set(batch_ids)
    page_cache = prefill_cache.reshape(LAYERS, N_BATCH, POSITIONS, 2, KV_HEADS, PAGE, HEAD)
    moved_pages = page_cache[:, sender_of, slot_ids[None, :]]
    keep_mask = in_use[sender_of, slot_ids[None, :]]
    decode_pool = jnp.where(keep_mask[None, :, :, None, None, None, None], moved_pages, jnp.zeros((), prefill_cache.dtype)).reshape(prefill_cache.shape)
    all_queries = queries.reshape(REQUESTS, LAYERS, STEPS, KV_HEADS, GROUP, HEAD)
    token_index = jnp.arange(PAGE, dtype=jnp.int32)
    step_index = jnp.arange(STEPS, dtype=jnp.int32)
    causal = step_index[None, :] <= step_index[:, None]
    layer_outputs = []
    for layer in range(LAYERS):
        layer_cache = page_cache[layer]
        layer_queries = all_queries[:, layer]

        def group_part(items):
            batch_row, use_row, request_row, live_row = items
            group_pages = lax.dynamic_index_in_dim(layer_cache, batch_row, 0, keepdims=False)
            group_queries = lax.dynamic_slice_in_dim(layer_queries, batch_row * REQ_GRP, REQ_GRP, 0)
            slot_queries = jnp.take(group_queries, request_row, axis=0)
            token_mask = token_index[None, None, None, None, :] < live_row[:, None, None, None, None]
            page_peak, weight_sum, page_output = block_partials(slot_queries, group_pages[:, 0], group_pages[:, 1], token_mask)
            mine = (request_row[None, :] == jnp.arange(REQ_GRP, dtype=jnp.int32)[:, None]) & use_row[None, :]
            row_mask = mine[:, :, None, None, None]
            request_peak = lax.optimization_barrier(jnp.max(jnp.where(row_mask, page_peak[None], MASKED), axis=1))
            factor = jnp.where(row_mask, jnp.exp(page_peak[None] - request_peak[:, None]), 0.0)
            numerator = jnp.einsum('rqgie,qgiex->rgiex', factor, page_output, precision=lax.Precision.HIGHEST)
            denominator = lax.optimization_barrier(jnp.sum(factor * weight_sum[None], axis=1))
            return (request_peak, numerator, denominator)
        request_peak, numerator, denominator = lax.map(group_part, (jnp.arange(N_BATCH, dtype=jnp.int32), in_use, request_of, live_count))
        request_peak = request_peak.reshape(REQUESTS, KV_HEADS, STEPS, GROUP)
        numerator = numerator.reshape(REQUESTS, KV_HEADS, STEPS, GROUP, HEAD)
        denominator = denominator.reshape(REQUESTS, KV_HEADS, STEPS, GROUP)
        new_keys = jnp.transpose(new_kv[:, layer, :, 0], (0, 2, 1, 3))
        new_values = jnp.transpose(new_kv[:, layer, :, 1], (0, 2, 1, 3))
        new_peak, new_sum, new_output = block_partials(layer_queries, new_keys, new_values, causal[None, None, :, None, :])
        joint_peak = jnp.maximum(request_peak, new_peak)
        old_scale = jnp.exp(request_peak - joint_peak)
        new_scale = jnp.exp(new_peak - joint_peak)
        result = (old_scale[..., None] * numerator + new_scale[..., None] * new_output) / (old_scale * denominator + new_scale * new_sum)[..., None]
        layer_outputs.append(jnp.transpose(result, (0, 2, 1, 3, 4)).reshape(REQUESTS, STEPS, Q_HEADS, HEAD))
    attended = jnp.stack(layer_outputs, axis=1).astype(jnp.bfloat16)
    return (attended, decode_pool)
```

```python
import math

import jax
import jax.numpy as jnp
from jax import lax
from jax.experimental import pallas as pl
from jax.experimental.pallas import tpu as pltpu
from jax.sharding import PartitionSpec as P

MASKED = -1e30


def partner_swap(value, axis, mask):
    pairs = [(source, source ^ mask) for source in range(lax.axis_size(axis))]
    return lax.ppermute(value, axis, pairs)


def page_partials(queries_at, key_rows, value_rows, token_mask):
    score_scale = 1.0 / math.sqrt(key_rows.shape[-1])
    scores = (
        jnp.einsum("nigex,ngpx->ngiep", queries_at, key_rows, preferred_element_type=jnp.float32)
        * score_scale
    )
    page_peak = jnp.max(jnp.where(token_mask, scores, MASKED), axis=-1)
    weights = jnp.where(token_mask, jnp.exp(scores - page_peak[..., None]), 0.0).astype(
        jnp.bfloat16
    )
    weight_sum = jnp.sum(weights.astype(jnp.float32), axis=-1)
    page_output = jnp.einsum(
        "ngiep,ngpx->ngiex", weights, value_rows, preferred_element_type=jnp.float32
    )
    return (page_peak, weight_sum, page_output)


def by_destination(keys, landed):
    batches, slots, heads, rows, width = landed.shape

    def body(keys_ref, landed_ref, out_ref):
        def step(dest, carry):
            for slot in range(slots):
                source = dest ^ keys_ref[slot]
                for head in range(heads):
                    out_ref[dest, head, slot] = landed_ref[source, slot, head]
            return carry

        lax.fori_loop(0, batches, step, 0, unroll=4)

    return pl.pallas_call(
        body,
        out_shape=jax.ShapeDtypeStruct((batches, heads, slots, rows, width), landed.dtype),
        in_specs=[
            pl.BlockSpec(memory_space=pltpu.SMEM),
            pl.BlockSpec(memory_space=pltpu.VMEM),
        ],
        out_specs=pl.BlockSpec(memory_space=pltpu.VMEM),
    )(keys, landed)


def on_device(prefill_cache, lengths, page_table, holder, queries, new_kv):
    batch_count, positions = holder.shape
    tensor_size = lax.axis_size("tensor")
    tensor_at = lax.axis_index("tensor")
    section_at = lax.axis_index("section")
    raw = prefill_cache[0]
    own_slots, kinds, heads, page_len, head_dim = raw.shape
    blocks = batch_count // kinds
    block_rows = page_len // blocks
    owned_rows, layers, step_count = (queries.shape[0], queries.shape[1], queries.shape[2])
    group_size = queries.shape[3]
    req_count, max_pages = page_table.shape

    slot_ids = jnp.arange(positions, dtype=jnp.int32)
    page_hits = (page_table[:, :, None] == slot_ids).astype(jnp.int32)
    in_use = jnp.sum(page_hits, axis=(0, 1)) > 0

    own_use = lax.dynamic_slice(in_use, (tensor_at * own_slots,), (own_slots,))
    own_keys = lax.dynamic_slice(holder[0], (tensor_at * own_slots,), (own_slots,))
    kept = jnp.where(own_use[:, None, None, None, None], raw, jnp.zeros((), raw.dtype))
    pieces = jnp.transpose(
        kept.reshape(own_slots, kinds, heads, blocks, block_rows, head_dim), (1, 3, 0, 2, 4, 5)
    ).reshape(batch_count, own_slots, heads, block_rows, head_dim)
    landed = lax.all_to_all(pieces, "batch", split_axis=0, concat_axis=0, tiled=True)

    outgoing = by_destination(own_keys, landed).reshape(
        batch_count * tensor_size, own_slots, block_rows, head_dim
    )
    arrived = lax.all_to_all(
        outgoing, ("batch", "tensor"), split_axis=0, concat_axis=0, tiled=True
    )
    decode_pool = jnp.transpose(
        arrived.reshape(batch_count, positions, block_rows, head_dim), (1, 0, 2, 3)
    ).reshape(1, positions, kinds, 1, page_len, head_dim)

    def head_of(index):
        return lax.dynamic_index_in_dim(raw, index, 2, keepdims=False)

    page_blocks = [head_of(tensor_at)]
    for mask in range(1, tensor_size):
        page_blocks.append(partner_swap(head_of(tensor_at ^ mask), "tensor", mask))
    local_pages = jnp.concatenate(page_blocks, axis=0)[:, :, None]
    slot_at = jnp.concatenate(
        [
            (tensor_at ^ mask) * own_slots + jnp.arange(own_slots, dtype=jnp.int32)
            for mask in range(tensor_size)
        ]
    )

    theirs = lax.dynamic_index_in_dim(queries, 1 - section_at, 1, keepdims=False)
    mine_q = lax.dynamic_index_in_dim(queries, section_at, 1, keepdims=False)
    got = partner_swap(theirs, "section", 1)
    first = section_at == 0
    local_queries = jnp.concatenate(
        [jnp.where(first, mine_q, got), jnp.where(first, got, mine_q)], axis=0
    ).reshape(req_count, step_count, 1, group_size, head_dim)

    hits = (page_table[:, :, None] == slot_at).astype(jnp.int32)
    used_at = jnp.sum(hits, axis=(0, 1)) > 0
    request_of = jnp.sum(
        hits * jnp.arange(req_count, dtype=jnp.int32)[:, None, None], axis=(0, 1)
    )
    page_of = jnp.sum(hits * jnp.arange(max_pages, dtype=jnp.int32)[None, :, None], axis=(0, 1))
    length_of = jnp.sum(hits * lengths[:, None, None], axis=(0, 1))
    live_count = jnp.clip(length_of - page_of * page_len, 0, page_len)
    position_queries = jnp.take(local_queries, request_of, axis=0)
    token_index = jnp.arange(page_len, dtype=jnp.int32)
    token_mask = token_index[None, None, None, None, :] < live_count[:, None, None, None, None]
    page_peak, weight_sum, page_output = page_partials(
        position_queries, local_pages[:, 0], local_pages[:, 1], token_mask
    )
    mine = (request_of[None, :] == jnp.arange(req_count, dtype=jnp.int32)[:, None]) & used_at[
        None, :
    ]
    row_mask = mine[:, :, None, None, None]
    request_peak = jnp.max(jnp.where(row_mask, page_peak[None], MASKED), axis=1)
    factor = jnp.where(row_mask, jnp.exp(page_peak[None] - request_peak[:, None]), 0.0)
    numerator = jnp.einsum(
        "rqgie,qgiex->rgiex", factor, page_output, precision=lax.Precision.HIGHEST
    )
    denominator = jnp.sum(factor * weight_sum[None], axis=1)

    merged = jnp.concatenate(
        [numerator, request_peak[..., None], denominator[..., None]], axis=-1
    )
    keep = lax.dynamic_slice_in_dim(merged, section_at * owned_rows, owned_rows, 0)
    give = lax.dynamic_slice_in_dim(merged, (1 - section_at) * owned_rows, owned_rows, 0)
    back = partner_swap(give, "section", 1)
    merged = jnp.stack([jnp.where(first, keep, back), jnp.where(first, back, keep)], axis=1)
    numerator = merged[..., :head_dim]
    request_peak = merged[..., head_dim]
    denominator = merged[..., head_dim + 1]

    flat_queries = queries.reshape(owned_rows * layers, step_count, 1, group_size, head_dim)
    new_keys = jnp.transpose(
        new_kv[:, :, :, 0].reshape(owned_rows * layers, step_count, 1, head_dim), (0, 2, 1, 3)
    )
    new_values = jnp.transpose(
        new_kv[:, :, :, 1].reshape(owned_rows * layers, step_count, 1, head_dim), (0, 2, 1, 3)
    )
    step_index = jnp.arange(step_count, dtype=jnp.int32)
    causal = step_index[None, :] <= step_index[:, None]
    new_peak, new_sum, new_output = page_partials(
        flat_queries, new_keys, new_values, causal[None, None, :, None, :]
    )
    new_peak = new_peak.reshape(request_peak.shape)
    new_sum = new_sum.reshape(denominator.shape)
    new_output = new_output.reshape(numerator.shape)
    joint_peak = jnp.maximum(request_peak, new_peak)
    old_scale = jnp.exp(request_peak - joint_peak)
    new_scale = jnp.exp(new_peak - joint_peak)
    result = (old_scale[..., None] * numerator + new_scale[..., None] * new_output) / (
        old_scale * denominator + new_scale * new_sum
    )[..., None]
    attended = (
        jnp.transpose(result, (0, 1, 3, 2, 4, 5))
        .reshape(owned_rows, layers, step_count, group_size, head_dim)
        .astype(jnp.bfloat16)
    )
    return (attended, decode_pool)


def solution(mesh):
    placed = (
        P("section", ("batch", "tensor"), None, None, None, None),
        P("batch"),
        P("batch", None),
        P(),
        P(("batch", "section"), None, None, "tensor", None),
        P(("batch", "section"), None, None, None, "tensor", None),
    )
    return jax.shard_map(
        on_device,
        mesh=mesh,
        in_specs=placed,
        out_specs=(
            P(("batch", "section"), None, None, "tensor", None),
            P("section", "batch", None, "tensor", None, None),
        ),
        check_vma=False,
    )
```

```python
import math

import jax
import jax.numpy as jnp
from jax import lax
from jax.experimental import pallas as pl
from jax.experimental.pallas import tpu as pltpu
from jax.sharding import PartitionSpec as P


MASKED = -1e30


def partner_swap(value, axis, mask):
    pairs = [(source, source ^ mask) for source in range(lax.axis_size(axis))]
    return lax.ppermute(value, axis, pairs)


def page_partials(queries_at, key_rows, value_rows, token_mask):
    score_scale = 1.0 / math.sqrt(key_rows.shape[-1])
    scores = (
        jnp.einsum("nigex,ngpx->ngiep", queries_at, key_rows, preferred_element_type=jnp.float32)
        * score_scale
    )
    page_peak = jnp.max(jnp.where(token_mask, scores, MASKED), axis=-1)
    weights = jnp.where(token_mask, jnp.exp(scores - page_peak[..., None]), 0.0).astype(
        jnp.bfloat16
    )
    weight_sum = jnp.sum(weights.astype(jnp.float32), axis=-1)
    page_output = jnp.einsum(
        "ngiep,ngpx->ngiex", weights, value_rows, preferred_element_type=jnp.float32
    )
    return (page_peak, weight_sum, page_output)


def by_destination(keys, landed):
    batches, slots, heads, rows, width = landed.shape

    def body(keys_ref, landed_ref, out_ref):
        def step(dest, carry):
            for slot in range(slots):
                source = dest ^ keys_ref[slot]
                for head in range(heads):
                    out_ref[dest, head, slot] = landed_ref[source, slot, head]
            return carry

        lax.fori_loop(0, batches, step, 0, unroll=4)

    return pl.pallas_call(
        body,
        out_shape=jax.ShapeDtypeStruct((batches, heads, slots, rows, width), landed.dtype),
        in_specs=[
            pl.BlockSpec(memory_space=pltpu.SMEM),
            pl.BlockSpec(memory_space=pltpu.VMEM),
        ],
        out_specs=pl.BlockSpec(memory_space=pltpu.VMEM),
        compiler_params=pltpu.CompilerParams(vmem_limit_bytes=4 * 2**20),
    )(keys, landed)


def pieces_to_spread(raw, page_table, blocks):
    slots, kinds, heads, page_len, width = raw.shape
    rows = page_len // blocks
    req_count, max_pages = page_table.shape
    parts = 2
    step_blocks = blocks // parts

    def body(table_ref, raw_ref, out_ref):
        first_slot = lax.axis_index("tensor") * slots
        for slot in range(slots):
            used = jnp.int32(0)
            for row in range(req_count):
                for column in range(max_pages):
                    hit = table_ref[row, column] == first_slot + slot
                    used = jnp.where(hit, jnp.int32(1), used)

            @pl.when(used > 0)
            def copy():
                for block in range(step_blocks):
                    for head in range(heads):
                        out_ref[block, slot, head] = raw_ref[
                            slot, 0, head, pl.ds(block * rows, rows)
                        ]

            @pl.when(used == 0)
            def clear():
                for block in range(step_blocks):
                    for head in range(heads):
                        out_ref[block, slot, head] = jnp.zeros((rows, width), raw.dtype)

    return pl.pallas_call(
        body,
        grid=(kinds, parts),
        out_shape=jax.ShapeDtypeStruct((kinds * blocks, slots, heads, rows, width), raw.dtype),
        in_specs=[
            pl.BlockSpec(memory_space=pltpu.SMEM),
            pl.BlockSpec(
                (slots, 1, heads, page_len // parts, width), lambda kind, part: (0, kind, 0, part, 0)
            ),
        ],
        out_specs=pl.BlockSpec(
            (step_blocks, slots, heads, rows, width),
            lambda kind, part: (kind * parts + part, 0, 0, 0, 0),
        ),
        compiler_params=pltpu.CompilerParams(vmem_limit_bytes=4 * 2**20),
    )(page_table, raw)


def on_device(prefill_cache, lengths, page_table, holder, queries, new_kv):
    batch_count, positions = holder.shape
    tensor_size = lax.axis_size("tensor")
    tensor_at = lax.axis_index("tensor")
    section_at = lax.axis_index("section")
    raw = prefill_cache[0]
    own_slots, kinds, _, page_len, head_dim = raw.shape
    blocks = batch_count // kinds
    block_rows = page_len // blocks
    owned_rows, layers, step_count = (queries.shape[0], queries.shape[1], queries.shape[2])
    group_size = queries.shape[3]
    req_count, max_pages = page_table.shape

    own_keys = lax.dynamic_slice(holder[0], (tensor_at * own_slots,), (own_slots,))
    pieces = pieces_to_spread(raw, page_table, blocks)
    landed = lax.all_to_all(pieces, "batch", split_axis=0, concat_axis=0, tiled=True)

    def head_of(index):
        return lax.dynamic_index_in_dim(raw, index, 2, keepdims=False)

    page_blocks = [head_of(tensor_at)]
    for mask in range(1, tensor_size):
        page_blocks.append(partner_swap(head_of(tensor_at ^ mask), "tensor", mask))
    outgoing = by_destination(own_keys, landed).reshape(
        batch_count * tensor_size, own_slots, block_rows, head_dim
    )
    local_pages = jnp.concatenate(page_blocks, axis=0)[:, :, None]
    slot_at = jnp.concatenate(
        [
            (tensor_at ^ mask) * own_slots + jnp.arange(own_slots, dtype=jnp.int32)
            for mask in range(tensor_size)
        ]
    )

    theirs = lax.dynamic_index_in_dim(queries, 1 - section_at, 1, keepdims=False)
    mine_q = lax.dynamic_index_in_dim(queries, section_at, 1, keepdims=False)
    got = partner_swap(theirs, "section", 1)
    first = section_at == 0
    local_queries = jnp.concatenate(
        [jnp.where(first, mine_q, got), jnp.where(first, got, mine_q)], axis=0
    ).reshape(req_count, step_count, 1, group_size, head_dim)

    hits = (page_table[:, :, None] == slot_at).astype(jnp.int32)
    used_at = jnp.sum(hits, axis=(0, 1)) > 0
    request_of = jnp.sum(
        hits * jnp.arange(req_count, dtype=jnp.int32)[:, None, None], axis=(0, 1)
    )
    page_of = jnp.sum(hits * jnp.arange(max_pages, dtype=jnp.int32)[None, :, None], axis=(0, 1))
    length_of = jnp.sum(hits * lengths[:, None, None], axis=(0, 1))
    live_count = jnp.clip(length_of - page_of * page_len, 0, page_len)
    position_queries = jnp.take(local_queries, request_of, axis=0)
    token_index = jnp.arange(page_len, dtype=jnp.int32)
    token_mask = token_index[None, None, None, None, :] < live_count[:, None, None, None, None]
    page_peak, weight_sum, page_output = page_partials(
        position_queries, local_pages[:, 0], local_pages[:, 1], token_mask
    )
    mine = (request_of[None, :] == jnp.arange(req_count, dtype=jnp.int32)[:, None]) & used_at[
        None, :
    ]
    row_mask = mine[:, :, None, None, None]
    request_peak = jnp.max(jnp.where(row_mask, page_peak[None], MASKED), axis=1)
    factor = jnp.where(row_mask, jnp.exp(page_peak[None] - request_peak[:, None]), 0.0)
    numerator = jnp.einsum(
        "rqgie,qgiex->rgiex", factor, page_output, precision=lax.Precision.HIGHEST
    )
    denominator = jnp.sum(factor * weight_sum[None], axis=1)

    merged = jnp.concatenate(
        [numerator, request_peak[..., None], denominator[..., None]], axis=-1
    )
    keep = lax.dynamic_slice_in_dim(merged, section_at * owned_rows, owned_rows, 0)
    give = lax.dynamic_slice_in_dim(merged, (1 - section_at) * owned_rows, owned_rows, 0)
    back = partner_swap(give, "section", 1)
    merged = jnp.stack([jnp.where(first, keep, back), jnp.where(first, back, keep)], axis=1)
    numerator = merged[..., :head_dim]
    request_peak = merged[..., head_dim]
    denominator = merged[..., head_dim + 1]

    flat_queries = queries.reshape(owned_rows * layers, step_count, 1, group_size, head_dim)
    new_keys = jnp.transpose(
        new_kv[:, :, :, 0].reshape(owned_rows * layers, step_count, 1, head_dim), (0, 2, 1, 3)
    )
    new_values = jnp.transpose(
        new_kv[:, :, :, 1].reshape(owned_rows * layers, step_count, 1, head_dim), (0, 2, 1, 3)
    )
    step_index = jnp.arange(step_count, dtype=jnp.int32)
    causal = step_index[None, :] <= step_index[:, None]
    new_peak, new_sum, new_output = page_partials(
        flat_queries, new_keys, new_values, causal[None, None, :, None, :]
    )
    new_peak = new_peak.reshape(request_peak.shape)
    new_sum = new_sum.reshape(denominator.shape)
    new_output = new_output.reshape(numerator.shape)
    joint_peak = jnp.maximum(request_peak, new_peak)
    old_scale = jnp.exp(request_peak - joint_peak)
    new_scale = jnp.exp(new_peak - joint_peak)
    result = (old_scale[..., None] * numerator + new_scale[..., None] * new_output) / (
        old_scale * denominator + new_scale * new_sum
    )[..., None]
    attended = (
        jnp.transpose(result, (0, 1, 3, 2, 4, 5))
        .reshape(owned_rows, layers, step_count, group_size, head_dim)
        .astype(jnp.bfloat16)
    )

    arrived = lax.all_to_all(outgoing, ("batch", "tensor"), split_axis=0, concat_axis=0, tiled=True)
    decode_pool = jnp.transpose(
        arrived.reshape(batch_count, positions, block_rows, head_dim), (1, 0, 2, 3)
    ).reshape(1, positions, kinds, 1, page_len, head_dim)
    return (attended, decode_pool)


def solution(mesh):
    placed = (
        P("section", ("batch", "tensor"), None, None, None, None),
        P("batch"),
        P("batch", None),
        P(),
        P(("batch", "section"), None, None, "tensor", None),
        P(("batch", "section"), None, None, None, "tensor", None),
    )

    return jax.shard_map(
        on_device,
        mesh=mesh,
        in_specs=placed,
        out_specs=(
            P(("batch", "section"), None, None, "tensor", None),
            P("section", "batch", None, "tensor", None, None),
        ),
        check_vma=False,
    )
```

```python
import math

import jax
import jax.numpy as jnp
from jax import lax
from jax.experimental import pallas as pl
from jax.experimental.pallas import tpu as pltpu
from jax.sharding import PartitionSpec as P


MASKED = -1e30


def partner_swap(value, axis, mask):
    pairs = [(source, source ^ mask) for source in range(lax.axis_size(axis))]
    return lax.ppermute(value, axis, pairs)


def page_partials(queries_at, key_rows, value_rows, token_mask):
    score_scale = 1.0 / math.sqrt(key_rows.shape[-1])
    scores = (
        jnp.einsum("nigex,ngpx->ngiep", queries_at, key_rows, preferred_element_type=jnp.float32)
        * score_scale
    )
    page_peak = jnp.max(jnp.where(token_mask, scores, MASKED), axis=-1)
    weights = jnp.where(token_mask, jnp.exp(scores - page_peak[..., None]), 0.0).astype(
        jnp.bfloat16
    )
    weight_sum = jnp.sum(weights.astype(jnp.float32), axis=-1)
    page_output = jnp.einsum(
        "ngiep,ngpx->ngiex", weights, value_rows, preferred_element_type=jnp.float32
    )
    return (page_peak, weight_sum, page_output)


def by_destination(key, landed):
    batches, heads, rows, width = landed.shape

    def body(key_ref, landed_ref, out_ref, ready, sent):
        def outward(head):
            return pltpu.make_async_copy(ready.at[head], out_ref.at[head], sent.at[head])

        for head in range(heads):

            def step(dest, carry):
                ready[head, dest] = landed_ref[dest ^ key_ref[0], head]
                return carry

            lax.fori_loop(0, batches, step, 0, unroll=16)
            outward(head).start()
        for head in range(heads):
            outward(head).wait()

    shape = (heads, batches, rows, width)
    return pl.pallas_call(
        body,
        out_shape=jax.ShapeDtypeStruct(shape, landed.dtype),
        in_specs=[
            pl.BlockSpec(memory_space=pltpu.SMEM),
            pl.BlockSpec(memory_space=pltpu.VMEM),
        ],
        out_specs=pl.BlockSpec(memory_space=pltpu.HBM),
        scratch_shapes=[pltpu.VMEM(shape, landed.dtype), pltpu.SemaphoreType.DMA((heads,))],
        compiler_params=pltpu.CompilerParams(vmem_limit_bytes=4 * 2**20),
    )(key, landed)


def pieces_to_spread(raw, page_table, rows):
    slots, kinds, heads, page_len, width = raw.shape
    blocks = page_len // rows
    req_count, max_pages = page_table.shape
    chunks = [(slot, kind) for slot in range(slots) for kind in range(kinds)]

    def body(table_ref, raw_ref, out_ref, table, here, ready, told, came, sent):
        def inward(slot, kind):
            return pltpu.make_async_copy(
                raw_ref.at[slot, kind], here.at[slot, kind], came.at[slot, kind]
            )

        def outward(slot, kind):
            return pltpu.make_async_copy(
                ready.at[slot, kind], out_ref.at[slot, kind], sent.at[slot, kind]
            )

        lookup = pltpu.make_async_copy(table_ref, table, told)
        lookup.start()
        for chunk in chunks:
            inward(*chunk).start()
        first_slot = lax.axis_index("tensor") * slots
        lookup.wait()
        used = []
        for slot in range(slots):
            found = jnp.int32(0)
            for row in range(req_count):
                for column in range(max_pages):
                    hit = table[row, column] == first_slot + slot
                    found = jnp.where(hit, jnp.int32(1), found)
            used.append(found > 0)
        empty = jnp.zeros((rows, width), raw.dtype)
        for slot, kind in chunks:
            inward(slot, kind).wait()
            for head in range(heads):
                for block in range(blocks):
                    piece = here[slot, kind, head, pl.ds(block * rows, rows)]
                    ready[slot, kind, block, head] = jnp.where(used[slot], piece, empty)
            outward(slot, kind).start()
        for chunk in chunks:
            outward(*chunk).wait()

    shape = (slots, kinds, blocks, heads, rows, width)
    return pl.pallas_call(
        body,
        out_shape=jax.ShapeDtypeStruct(shape, raw.dtype),
        in_specs=[
            pl.BlockSpec(memory_space=pltpu.HBM),
            pl.BlockSpec(memory_space=pltpu.HBM),
        ],
        out_specs=pl.BlockSpec(memory_space=pltpu.HBM),
        scratch_shapes=[
            pltpu.SMEM(page_table.shape, page_table.dtype),
            pltpu.VMEM(raw.shape, raw.dtype),
            pltpu.VMEM(shape, raw.dtype),
            pltpu.SemaphoreType.DMA,
            pltpu.SemaphoreType.DMA((slots, kinds)),
            pltpu.SemaphoreType.DMA((slots, kinds)),
        ],
        compiler_params=pltpu.CompilerParams(vmem_limit_bytes=63 * 2**20),
    )(page_table, raw)


def on_device(prefill_cache, lengths, page_table, holder, queries, new_kv):
    batch_count, positions = holder.shape
    tensor_size = lax.axis_size("tensor")
    tensor_at = lax.axis_index("tensor")
    section_at = lax.axis_index("section")
    raw = prefill_cache[0]
    own_slots, kinds, heads, page_len, head_dim = raw.shape
    piece_rows = own_slots * kinds * page_len // batch_count
    owned_rows, layers, step_count = (queries.shape[0], queries.shape[1], queries.shape[2])
    group_size = queries.shape[3]
    req_count, max_pages = page_table.shape

    spread_at = lax.axis_index("batch") // (batch_count // own_slots)
    relayed_key = lax.dynamic_slice(holder, (0, tensor_at * own_slots + spread_at), (1, 1))
    pieces = pieces_to_spread(raw, page_table, piece_rows).reshape(
        batch_count, heads, piece_rows, head_dim
    )
    landed = lax.all_to_all(pieces, "batch", split_axis=0, concat_axis=0, tiled=True)
    outgoing = by_destination(relayed_key.reshape(1), landed).reshape(
        tensor_size * batch_count, piece_rows, head_dim
    )

    def head_of(index):
        return lax.dynamic_index_in_dim(raw, index, 2, keepdims=False)

    page_blocks = [head_of(tensor_at)]
    for mask in range(1, tensor_size):
        page_blocks.append(partner_swap(head_of(tensor_at ^ mask), "tensor", mask))
    local_pages = jnp.concatenate(page_blocks, axis=0)[:, :, None]
    slot_at = jnp.concatenate(
        [
            (tensor_at ^ mask) * own_slots + jnp.arange(own_slots, dtype=jnp.int32)
            for mask in range(tensor_size)
        ]
    )

    theirs = lax.dynamic_index_in_dim(queries, 1 - section_at, 1, keepdims=False)
    mine_q = lax.dynamic_index_in_dim(queries, section_at, 1, keepdims=False)
    got = partner_swap(theirs, "section", 1)
    first = section_at == 0
    local_queries = jnp.concatenate(
        [jnp.where(first, mine_q, got), jnp.where(first, got, mine_q)], axis=0
    ).reshape(req_count, step_count, 1, group_size, head_dim)

    hits = (page_table[:, :, None] == slot_at).astype(jnp.int32)
    used_at = jnp.sum(hits, axis=(0, 1)) > 0
    request_of = jnp.sum(
        hits * jnp.arange(req_count, dtype=jnp.int32)[:, None, None], axis=(0, 1)
    )
    page_of = jnp.sum(hits * jnp.arange(max_pages, dtype=jnp.int32)[None, :, None], axis=(0, 1))
    length_of = jnp.sum(hits * lengths[:, None, None], axis=(0, 1))
    live_count = jnp.clip(length_of - page_of * page_len, 0, page_len)
    position_queries = jnp.take(local_queries, request_of, axis=0)
    token_index = jnp.arange(page_len, dtype=jnp.int32)
    token_mask = token_index[None, None, None, None, :] < live_count[:, None, None, None, None]
    page_peak, weight_sum, page_output = page_partials(
        position_queries, local_pages[:, 0], local_pages[:, 1], token_mask
    )
    mine = (request_of[None, :] == jnp.arange(req_count, dtype=jnp.int32)[:, None]) & used_at[
        None, :
    ]
    row_mask = mine[:, :, None, None, None]
    request_peak = jnp.max(jnp.where(row_mask, page_peak[None], MASKED), axis=1)
    factor = jnp.where(row_mask, jnp.exp(page_peak[None] - request_peak[:, None]), 0.0)
    numerator = jnp.einsum(
        "rqgie,qgiex->rgiex", factor, page_output, precision=lax.Precision.HIGHEST
    )
    denominator = jnp.sum(factor * weight_sum[None], axis=1)

    merged = jnp.concatenate(
        [numerator, request_peak[..., None], denominator[..., None]], axis=-1
    )
    keep = lax.dynamic_slice_in_dim(merged, section_at * owned_rows, owned_rows, 0)
    give = lax.dynamic_slice_in_dim(merged, (1 - section_at) * owned_rows, owned_rows, 0)
    back = partner_swap(give, "section", 1)
    merged = jnp.stack([jnp.where(first, keep, back), jnp.where(first, back, keep)], axis=1)
    numerator = merged[..., :head_dim]
    request_peak = merged[..., head_dim]
    denominator = merged[..., head_dim + 1]

    flat_queries = queries.reshape(owned_rows * layers, step_count, 1, group_size, head_dim)
    new_keys = jnp.transpose(
        new_kv[:, :, :, 0].reshape(owned_rows * layers, step_count, 1, head_dim), (0, 2, 1, 3)
    )
    new_values = jnp.transpose(
        new_kv[:, :, :, 1].reshape(owned_rows * layers, step_count, 1, head_dim), (0, 2, 1, 3)
    )
    step_index = jnp.arange(step_count, dtype=jnp.int32)
    causal = step_index[None, :] <= step_index[:, None]
    new_peak, new_sum, new_output = page_partials(
        flat_queries, new_keys, new_values, causal[None, None, :, None, :]
    )
    new_peak = new_peak.reshape(request_peak.shape)
    new_sum = new_sum.reshape(denominator.shape)
    new_output = new_output.reshape(numerator.shape)
    joint_peak = jnp.maximum(request_peak, new_peak)
    old_scale = jnp.exp(request_peak - joint_peak)
    new_scale = jnp.exp(new_peak - joint_peak)
    result = (old_scale[..., None] * numerator + new_scale[..., None] * new_output) / (
        old_scale * denominator + new_scale * new_sum
    )[..., None]
    attended = (
        jnp.transpose(result, (0, 1, 3, 2, 4, 5))
        .reshape(owned_rows, layers, step_count, group_size, head_dim)
        .astype(jnp.bfloat16)
    )

    arrived = lax.all_to_all(outgoing, ("tensor", "batch"), split_axis=0, concat_axis=0, tiled=True)
    decode_pool = arrived.reshape(1, positions, kinds, 1, page_len, head_dim)
    return (attended, decode_pool)


def solution(mesh):
    placed = (
        P("section", ("batch", "tensor"), None, None, None, None),
        P("batch"),
        P("batch", None),
        P(),
        P(("batch", "section"), None, None, "tensor", None),
        P(("batch", "section"), None, None, None, "tensor", None),
    )

    return jax.shard_map(
        on_device,
        mesh=mesh,
        in_specs=placed,
        out_specs=(
            P(("batch", "section"), None, None, "tensor", None),
            P("section", "batch", None, "tensor", None, None),
        ),
        check_vma=False,
    )
```

```python
import math

import jax
import jax.numpy as jnp
from jax import lax
from jax.experimental import pallas as pl
from jax.experimental.pallas import tpu as pltpu
from jax.sharding import PartitionSpec as P


MASKED = -1e30


def partner_swap(value, axis, mask):
    pairs = [(source, source ^ mask) for source in range(lax.axis_size(axis))]
    return lax.ppermute(value, axis, pairs)


def page_partials(queries_at, key_rows, value_rows, token_mask):
    score_scale = 1.0 / math.sqrt(key_rows.shape[-1])
    scores = (
        jnp.einsum("nigex,ngpx->ngiep", queries_at, key_rows, preferred_element_type=jnp.float32)
        * score_scale
    )
    page_peak = jnp.max(jnp.where(token_mask, scores, MASKED), axis=-1)
    weights = jnp.where(token_mask, jnp.exp(scores - page_peak[..., None]), 0.0).astype(
        jnp.bfloat16
    )
    weight_sum = jnp.sum(weights.astype(jnp.float32), axis=-1)
    page_output = jnp.einsum(
        "ngiep,ngpx->ngiex", weights, value_rows, preferred_element_type=jnp.float32
    )
    return (page_peak, weight_sum, page_output)


def by_destination(key, landed):
    batches, heads, rows, width = landed.shape

    def body(key_ref, landed_ref, out_ref, ready, sent):
        def outward(head):
            return pltpu.make_async_copy(ready.at[head], out_ref.at[head], sent.at[head])

        own_key = jnp.max(key_ref[...])
        for head in range(heads):

            def step(dest, carry):
                ready[head, dest] = landed_ref[dest ^ own_key, head]
                return carry

            lax.fori_loop(0, batches, step, 0, unroll=16)
            outward(head).start()
        for head in range(heads):
            outward(head).wait()

    shape = (heads, batches, rows, width)
    return pl.pallas_call(
        body,
        out_shape=jax.ShapeDtypeStruct(shape, landed.dtype),
        in_specs=[
            pl.BlockSpec(memory_space=pltpu.VMEM),
            pl.BlockSpec(memory_space=pltpu.VMEM),
        ],
        out_specs=pl.BlockSpec(memory_space=pltpu.HBM),
        scratch_shapes=[pltpu.VMEM(shape, landed.dtype), pltpu.SemaphoreType.DMA((heads,))],
        compiler_params=pltpu.CompilerParams(vmem_limit_bytes=4 * 2**20),
    )(key, landed)


def pieces_to_spread(raw, page_table, rows):
    slots, kinds, heads, page_len, width = raw.shape
    blocks = page_len // rows
    req_count, max_pages = page_table.shape
    chunks = [(slot, kind) for slot in range(slots) for kind in range(kinds)]

    def body(table_ref, raw_ref, out_ref, table, here, ready, told, came, sent):
        def inward(slot, kind):
            return pltpu.make_async_copy(
                raw_ref.at[slot, kind], here.at[slot, kind], came.at[slot, kind]
            )

        def outward(slot, kind):
            return pltpu.make_async_copy(
                ready.at[slot, kind], out_ref.at[slot, kind], sent.at[slot, kind]
            )

        lookup = pltpu.make_async_copy(table_ref, table, told)
        lookup.start()
        for chunk in chunks:
            inward(*chunk).start()
        first_slot = lax.axis_index("tensor") * slots
        lookup.wait()
        used = []
        for slot in range(slots):
            found = jnp.int32(0)
            for row in range(req_count):
                for column in range(max_pages):
                    hit = table[row, column] == first_slot + slot
                    found = jnp.where(hit, jnp.int32(1), found)
            used.append(found > 0)
        empty = jnp.zeros((rows, width), raw.dtype)
        for slot, kind in chunks:
            inward(slot, kind).wait()
            for head in range(heads):
                for block in range(blocks):
                    piece = here[slot, kind, head, pl.ds(block * rows, rows)]
                    ready[slot, kind, block, head] = jnp.where(used[slot], piece, empty)
            outward(slot, kind).start()
        for chunk in chunks:
            outward(*chunk).wait()

    shape = (slots, kinds, blocks, heads, rows, width)
    return pl.pallas_call(
        body,
        out_shape=jax.ShapeDtypeStruct(shape, raw.dtype),
        in_specs=[
            pl.BlockSpec(memory_space=pltpu.HBM),
            pl.BlockSpec(memory_space=pltpu.HBM),
        ],
        out_specs=pl.BlockSpec(memory_space=pltpu.HBM),
        scratch_shapes=[
            pltpu.SMEM(page_table.shape, page_table.dtype),
            pltpu.VMEM(raw.shape, raw.dtype),
            pltpu.VMEM(shape, raw.dtype),
            pltpu.SemaphoreType.DMA,
            pltpu.SemaphoreType.DMA((slots, kinds)),
            pltpu.SemaphoreType.DMA((slots, kinds)),
        ],
        compiler_params=pltpu.CompilerParams(vmem_limit_bytes=63 * 2**20),
    )(page_table, raw)


def on_device(prefill_cache, lengths, page_table, holder, queries, new_kv):
    batch_count, positions = holder.shape
    tensor_size = lax.axis_size("tensor")
    tensor_at = lax.axis_index("tensor")
    section_at = lax.axis_index("section")
    raw = prefill_cache[0]
    own_slots, kinds, heads, page_len, head_dim = raw.shape
    piece_rows = own_slots * kinds * page_len // batch_count
    owned_rows, layers, step_count = (queries.shape[0], queries.shape[1], queries.shape[2])
    group_size = queries.shape[3]
    req_count, max_pages = page_table.shape

    spread_at = lax.axis_index("batch") // (batch_count // own_slots)
    relayed_key = lax.dynamic_slice(holder, (0, tensor_at * own_slots + spread_at), (1, 1))
    pieces = pieces_to_spread(raw, page_table, piece_rows).reshape(
        batch_count, heads, piece_rows, head_dim
    )
    landed = lax.all_to_all(pieces, "batch", split_axis=0, concat_axis=0, tiled=True)
    outgoing = by_destination(jnp.broadcast_to(relayed_key, (8, 128)), landed).reshape(
        tensor_size * batch_count, piece_rows, head_dim
    )

    def head_of(index):
        return lax.dynamic_index_in_dim(raw, index, 2, keepdims=False)

    page_blocks = [head_of(tensor_at)]
    for mask in range(1, tensor_size):
        page_blocks.append(partner_swap(head_of(tensor_at ^ mask), "tensor", mask))
    local_pages = jnp.concatenate(page_blocks, axis=0)[:, :, None]
    slot_at = jnp.concatenate(
        [
            (tensor_at ^ mask) * own_slots + jnp.arange(own_slots, dtype=jnp.int32)
            for mask in range(tensor_size)
        ]
    )

    theirs = lax.dynamic_index_in_dim(queries, 1 - section_at, 1, keepdims=False)
    mine_q = lax.dynamic_index_in_dim(queries, section_at, 1, keepdims=False)
    got = partner_swap(theirs, "section", 1)
    first = section_at == 0
    local_queries = jnp.concatenate(
        [jnp.where(first, mine_q, got), jnp.where(first, got, mine_q)], axis=0
    ).reshape(req_count, step_count, 1, group_size, head_dim)

    hits = (page_table[:, :, None] == slot_at).astype(jnp.int32)
    used_at = jnp.sum(hits, axis=(0, 1)) > 0
    request_of = jnp.sum(
        hits * jnp.arange(req_count, dtype=jnp.int32)[:, None, None], axis=(0, 1)
    )
    page_of = jnp.sum(hits * jnp.arange(max_pages, dtype=jnp.int32)[None, :, None], axis=(0, 1))
    length_of = jnp.sum(hits * lengths[:, None, None], axis=(0, 1))
    live_count = jnp.clip(length_of - page_of * page_len, 0, page_len)
    position_queries = jnp.take(local_queries, request_of, axis=0)
    token_index = jnp.arange(page_len, dtype=jnp.int32)
    token_mask = token_index[None, None, None, None, :] < live_count[:, None, None, None, None]
    page_peak, weight_sum, page_output = page_partials(
        position_queries, local_pages[:, 0], local_pages[:, 1], token_mask
    )
    mine = (request_of[None, :] == jnp.arange(req_count, dtype=jnp.int32)[:, None]) & used_at[
        None, :
    ]
    row_mask = mine[:, :, None, None, None]
    request_peak = jnp.max(jnp.where(row_mask, page_peak[None], MASKED), axis=1)
    factor = jnp.where(row_mask, jnp.exp(page_peak[None] - request_peak[:, None]), 0.0)
    numerator = jnp.einsum(
        "rqgie,qgiex->rgiex", factor, page_output, precision=lax.Precision.HIGHEST
    )
    denominator = jnp.sum(factor * weight_sum[None], axis=1)

    merged = jnp.concatenate(
        [numerator, request_peak[..., None], denominator[..., None]], axis=-1
    )
    keep = lax.dynamic_slice_in_dim(merged, section_at * owned_rows, owned_rows, 0)
    give = lax.dynamic_slice_in_dim(merged, (1 - section_at) * owned_rows, owned_rows, 0)
    back = partner_swap(give, "section", 1)
    merged = jnp.stack([jnp.where(first, keep, back), jnp.where(first, back, keep)], axis=1)
    numerator = merged[..., :head_dim]
    request_peak = merged[..., head_dim]
    denominator = merged[..., head_dim + 1]

    flat_queries = queries.reshape(owned_rows * layers, step_count, 1, group_size, head_dim)
    new_keys = jnp.transpose(
        new_kv[:, :, :, 0].reshape(owned_rows * layers, step_count, 1, head_dim), (0, 2, 1, 3)
    )
    new_values = jnp.transpose(
        new_kv[:, :, :, 1].reshape(owned_rows * layers, step_count, 1, head_dim), (0, 2, 1, 3)
    )
    step_index = jnp.arange(step_count, dtype=jnp.int32)
    causal = step_index[None, :] <= step_index[:, None]
    new_peak, new_sum, new_output = page_partials(
        flat_queries, new_keys, new_values, causal[None, None, :, None, :]
    )
    new_peak = new_peak.reshape(request_peak.shape)
    new_sum = new_sum.reshape(denominator.shape)
    new_output = new_output.reshape(numerator.shape)
    joint_peak = jnp.maximum(request_peak, new_peak)
    old_scale = jnp.exp(request_peak - joint_peak)
    new_scale = jnp.exp(new_peak - joint_peak)
    result = (old_scale[..., None] * numerator + new_scale[..., None] * new_output) / (
        old_scale * denominator + new_scale * new_sum
    )[..., None]
    attended = (
        jnp.transpose(result, (0, 1, 3, 2, 4, 5))
        .reshape(owned_rows, layers, step_count, group_size, head_dim)
        .astype(jnp.bfloat16)
    )

    arrived = lax.all_to_all(outgoing, ("tensor", "batch"), split_axis=0, concat_axis=0, tiled=True)
    decode_pool = arrived.reshape(1, positions, kinds, 1, page_len, head_dim)
    return (attended, decode_pool)


def solution(mesh):
    placed = (
        P("section", ("batch", "tensor"), None, None, None, None),
        P("batch"),
        P("batch", None),
        P(),
        P(("batch", "section"), None, None, "tensor", None),
        P(("batch", "section"), None, None, None, "tensor", None),
    )

    return jax.shard_map(
        on_device,
        mesh=mesh,
        in_specs=placed,
        out_specs=(
            P(("batch", "section"), None, None, "tensor", None),
            P("section", "batch", None, "tensor", None, None),
        ),
        check_vma=False,
    )
```
